32 devices in a mesh: replica: 4 (over y, core), shard: 8 (over z, x).
Axes of the slice: x: 2, y: 2, z: 4, core: 2. Of those that a mesh axis runs over, the one named last changes fastest.
Arguments:
- inputs: bfloat16 [512, 2048], P('replica'), may hold values from -6 to 6
- gate_pre: bfloat16 [512, 8192], P('replica', 'shard'), may hold values from -8 to 8
- up_pre: bfloat16 [512, 8192], P('replica', 'shard'), may hold values from -6 to 6
- hidden_grad: bfloat16 [512, 8192], P('replica', 'shard'), may hold values from -6 to 6
- segment_ids: int32 [4, 128], P('replica'), may hold values from 0 to 15, never falling along the last dimension, each value on 1 to 32 neighbouring positions
- doc_weight: int32 [4, 16], P('replica'), may hold values from 1 to 12
- w_gate: bfloat16 [2048, 8192], P(None, 'shard'), may hold values from -0.0625 to 0.0625
- master: float32 [2048, 8192], P('replica', 'shard'), may hold values from -6 to 6
- moment: float32 [2048, 8192], P('replica', 'shard'), may hold values from -10 to 10
- second: float32 [2048, 8192], P('replica', 'shard'), may hold values from 0.5 to 20
Outputs:
- input_grad: bfloat16 [512, 2048], P(('replica', 'shard'))
- up_grad: bfloat16 [512, 8192], P('replica', 'shard')
- master_new: float32 [2048, 8192], P('replica', 'shard')
- moment_new: float32 [2048, 8192], P('replica', 'shard')
- second_new: float32 [2048, 8192], P('replica', 'shard')
The draws below stay inside these ranges and needn't reach their ends.
Inputs may be any that keep to these rules, and one draw needn't show every extreme that they name: `segment_ids`: within each group the documents occupy runs of positions numbered 0 to 15 in order, each at most 32 long.
All inputs are finite; a program needn't handle non-finite values.
Results may differ from the reference program's by a relative error of at most 0.0049.
Values sent between devices are 32-bit elements; how exact they have to be, the bound alone decides.
A program may use at most 64 MiB of HBM per device.

```python
import math
import jax
import jax.numpy as jnp
import numpy as np
from jax import lax

DW = 2048
FF = 8192
SEGS = 16
GROUP_TOK = 128
TOKENS = 512
N_REPLICA = 4


def draw_doc_weight(key, part):
    base_key = jax.random.fold_in(key, 11)
    start_key = jax.random.fold_in(key, 12)
    length_key = jax.random.fold_in(key, 13)
    base = jax.random.randint(base_key, (N_REPLICA, SEGS), 1, 4)
    groups = jnp.arange(N_REPLICA, dtype=jnp.int32)
    labels = jnp.arange(SEGS, dtype=jnp.int32)
    first_cell = (groups[:, None] == 0) & (labels[None, :] == 0)
    last_cell = (groups[:, None] == N_REPLICA - 1) & (labels[None, :] == 0)
    base = jnp.where(first_cell, 1, base)
    base = jnp.where(last_cell, 3, base)
    rising = 8 * groups // N_REPLICA
    window_start = jax.random.randint(start_key, (), 0, N_REPLICA)
    window_length = jax.random.randint(length_key, (), 0, N_REPLICA + 1)
    inside = (jnp.mod(groups - window_start, N_REPLICA) < window_length).astype(jnp.int32)
    inside = jnp.where(groups == 0, 0, inside)
    inside = jnp.where(groups == N_REPLICA - 1, 1, inside)
    return (base + rising[:, None] + 3 * inside[:, None]).astype(jnp.int32)


def spiked(result, stream_key, source, target, blocks, factor):
    def block_of(position):
        return (jnp.arange(result.shape[position]) // (result.shape[position] // blocks)).reshape((-1,) + (1,) * (result.ndim - 1 - position))

    one_side = jax.random.permutation(stream_key, blocks)[block_of(target)]
    other_side = (block_of(target) + blocks // 2) % blocks
    return jnp.where((block_of(source) == one_side) | (block_of(source) == other_side), factor * result, result)


def shard_levels(own_key, dims, cuts, smallest, largest):
    def one(axis_at, parts):
        steps = jax.random.uniform(jax.random.fold_in(jax.random.fold_in(own_key, 6), axis_at), (parts,), jnp.float32, smallest / len(cuts), largest / len(cuts))
        return jnp.repeat(jnp.exp(steps), dims[axis_at] // parts).reshape((-1,) + (1,) * (len(dims) - axis_at - 1))

    gain = one(*cuts[0])
    for cut in cuts[1:]:
        gain = gain * one(*cut)
    return gain


def split_up(count, total, limit, skew):
    loads = [(1 << 20) // math.isqrt(grade ** skew) + 1 for grade in range(2, count + 1)]
    surplus, holding = total - limit - (count - 1), [1] * (count - 1)
    while surplus > 0:
        free = [i for i in range(count - 1) if holding[i] < limit]
        mass, remaining = sum([loads[i] for i in free]), surplus
        for i in free:
            more = min(limit - holding[i], max(1, remaining * loads[i] // mass), surplus)
            holding[i] = holding[i] + more
            surplus = surplus - more
    return np.array([limit] + holding)


def ragged(stream_key, amount, total, bound, slope):
    if amount == 2:
        one = jax.random.randint(stream_key, (), max(1, total - bound), min(bound, total - 1) + 1)
        return jnp.stack([one, total - one])
    tallies = jnp.asarray(split_up(amount, total, bound, slope), jnp.int32)
    couples = (amount - 1) // 2
    giver, receiver = tallies[1:1 + 2 * couples:2], tallies[2:2 + 2 * couples:2]
    margin = jnp.minimum(giver - 1, bound - receiver)
    moved = jax.random.randint(jax.random.fold_in(stream_key, 1), (couples,), 0, 1 << 20) % (margin + 1)
    tallies = tallies.at[1:1 + 2 * couples:2].set(giver - moved).at[2:2 + 2 * couples:2].set(receiver + moved)
    return tallies[jax.random.permutation(jax.random.fold_in(stream_key, 2), amount)]


def noise(rng, shape, spread, reach, pieces=(), kind=jnp.bfloat16):
    loudness = shard_levels(rng, shape, pieces, -0.22, 0.18) if pieces else 1.0
    values = jax.random.normal(rng, shape, jnp.float32) * spread * loudness
    return jnp.minimum(jnp.maximum(values, -reach), reach).astype(kind)


def heavy_noise(rng, shape, deviation, limit, split, heavy, kind=jnp.bfloat16):
    drawn = deviation * jax.random.normal(rng, shape, jnp.float32)
    if split:
        drawn = drawn * shard_levels(rng, shape, split, -0.22, 0.18)
    return jnp.clip(spiked(drawn, jax.random.fold_in(rng, 3), *heavy), -limit, limit).astype(kind)


def setup_inputs(seed: int = 0) -> dict:
    keys = jax.random.split(jax.random.key(seed), 11)
    return {
        "inputs": heavy_noise(keys[0], (TOKENS, DW), 1.0, 6.0, ((0, 4),), (0, 1, 4, 2.0)),
        "gate_pre": noise(keys[1], (TOKENS, FF), 2.0, 8.0, ((0, 4), (1, 8))),
        "up_pre": noise(keys[2], (TOKENS, FF), 1.0, 6.0, ((0, 4), (1, 8))),
        "hidden_grad": heavy_noise(keys[3], (TOKENS, FF), 1.0, 6.0, ((0, 4), (1, 8)), (1, 0, 8, 2.0)),
        "segment_ids": jax.vmap(lambda own: jnp.searchsorted(jnp.cumsum(ragged(own, SEGS, GROUP_TOK, GROUP_TOK // 4, 2)), jnp.arange(GROUP_TOK), side="right"))(jax.random.split(keys[4], N_REPLICA)).reshape((N_REPLICA, GROUP_TOK)).astype(jnp.int32),
        "doc_weight": draw_doc_weight(jax.random.fold_in(keys[10], 71), 0),
        "w_gate": noise(keys[6], (DW, FF), FF ** -0.5, 0.0625, ((1, 8),)),
        "master": noise(keys[7], (DW, FF), 1.0, 6.0, ((0, 4), (1, 8)), jnp.float32),
        "moment": noise(keys[8], (DW, FF), 2.0, 10.0, ((0, 4), (1, 8)), jnp.float32),
        "second": jnp.clip(jnp.exp(math.log(20.0) - 3.6888795 * jax.random.uniform(keys[9], (DW, FF), jnp.float32) ** shard_levels(keys[9], (DW, FF), ((0, 4), (1, 8)), -0.2, 0.2)), 0.5, 20.0),
    }


def token_weights(segment_ids, doc_weight):
    labels = jnp.arange(doc_weight.shape[1], dtype=jnp.int32)
    onehot = segment_ids[:, :, None] == labels[None, None, :]
    return lax.optimization_barrier(jnp.sum(jnp.where(onehot, doc_weight[:, None, :], 0), axis=2)).astype(jnp.int32)

def reference(inputs, gate_pre, up_pre, hidden_grad, segment_ids, doc_weight, w_gate, master, moment, second):
    weights = token_weights(segment_ids, doc_weight)
    total = jnp.sum(weights).astype(jnp.int32)
    total_f = total.astype(jnp.float32)
    scale = jnp.float32(TOKENS) / total_f
    group_scale = jnp.float32(GROUP_TOK) / total_f
    stacked = (inputs.reshape(N_REPLICA, GROUP_TOK, DW), gate_pre.reshape(N_REPLICA, GROUP_TOK, FF), up_pre.reshape(N_REPLICA, GROUP_TOK, FF), hidden_grad.reshape(N_REPLICA, GROUP_TOK, FF), weights)

    def one_group(accum, block):
        rows, gate_blk, up_blk, grad_blk, weight_blk = block
        gate_f = gate_blk.astype(jnp.float32)
        sigmoid_gate = jax.nn.sigmoid(gate_f)
        weighted = grad_blk.astype(jnp.float32) * weight_blk.astype(jnp.float32)[:, None]
        gate_raw = (weighted * up_blk.astype(jnp.float32) * sigmoid_gate * (1.0 + gate_f * (1.0 - sigmoid_gate))).astype(jnp.bfloat16)
        up_out = (weighted * gate_f * sigmoid_gate * scale).astype(jnp.bfloat16)
        input_part = lax.dot_general(gate_raw, w_gate, (((1,), (1,)), ((), ())), preferred_element_type=jnp.float32)
        input_out = (input_part * scale).astype(jnp.bfloat16)
        accum = accum + lax.dot_general(rows, gate_raw, (((0,), (0,)), ((), ())), preferred_element_type=jnp.float32)
        return (accum, (input_out, up_out))
    start = jnp.zeros((DW, FF), jnp.float32)
    weight_raw, (input_grad, up_grad) = lax.scan(one_group, start, stacked)
    grad = weight_raw * group_scale
    moment_new = 0.9 * moment + 0.1 * grad
    second_new = 0.95 * second + 0.05 * grad * grad
    first_fix = moment_new / (1.0 - 0.9 ** 8)
    second_fix = second_new / (1.0 - 0.95 ** 8)
    master_new = master - 0.003 * (first_fix / (jnp.sqrt(second_fix) + 1e-08) + 0.1 * master)
    return (input_grad.reshape(TOKENS, DW), up_grad.reshape(TOKENS, FF), master_new, moment_new, second_new)
```

```python
import functools

import jax
import jax.numpy as jnp
from jax import lax
from jax.experimental import pallas as pl
from jax.experimental.pallas import tpu as pltpu
from jax.sharding import PartitionSpec as P

MESH = pl.DeviceIdType.MESH
QUARTERS = 4


def token_weights(segment_ids, doc_weight):
    labels = jnp.arange(doc_weight.shape[1], dtype=jnp.int32)
    onehot = segment_ids[:, :, None] == labels[None, None, :]
    return jnp.sum(jnp.where(onehot, doc_weight[:, None, :], 0), axis=2)


def adamw(grad, master, moment, second):
    moment_new = 0.9 * moment + 0.1 * grad
    second_new = 0.95 * second + 0.05 * grad * grad
    first_fix = moment_new / (1.0 - 0.9**8)
    second_fix = second_new / (1.0 - 0.95**8)
    master_new = master - 0.003 * (first_fix / (jnp.sqrt(second_fix) + 1e-08) + 0.1 * master)
    return master_new, moment_new, second_new


def reduce_path(
    inputs, gate_pre, up_pre, hidden_grad, segment_ids, doc_weight, w_gate, master, moment, second
):
    group_rows = inputs.shape[0]
    replicas = lax.axis_size("replica")
    weights = token_weights(segment_ids, doc_weight)[0]
    local_count = jnp.sum(weights)
    gate_f = gate_pre.astype(jnp.float32)
    sigmoid_gate = jax.nn.sigmoid(gate_f)
    weighted = hidden_grad.astype(jnp.float32) * weights.astype(jnp.float32)[:, None]
    gate_raw = (
        weighted * up_pre.astype(jnp.float32) * sigmoid_gate * (1.0 + gate_f * (1.0 - sigmoid_gate))
    ).astype(jnp.bfloat16)
    up_part = weighted * gate_f * sigmoid_gate
    input_part = lax.dot_general(
        gate_raw, w_gate, (((1,), (1,)), ((), ())), preferred_element_type=jnp.float32
    )
    input_summed = lax.psum_scatter(input_part, "shard", scatter_dimension=0, tiled=True)
    total = lax.psum(local_count, "replica").astype(jnp.float32)
    summed_grad = lax.psum_scatter(
        lax.dot_general(
            inputs, gate_raw, (((0,), (0,)), ((), ())), preferred_element_type=jnp.float32
        ),
        "replica",
        scatter_dimension=0,
        tiled=True,
    )
    scale = jnp.float32(group_rows * replicas) / total
    group_scale = jnp.float32(group_rows) / total
    input_grad = (input_summed * scale).astype(jnp.bfloat16)
    up_grad = (up_part * scale).astype(jnp.bfloat16)
    return (input_grad, up_grad) + adamw(summed_grad * group_scale, master, moment, second)


def flip(index, bit):
    return index + bit - 2 * bit * lax.rem(lax.div(index, bit), 2)


def exchange_kernel(
    x_hbm, gate_hbm, up_hbm, hid_hbm, seg_hbm, dw_hbm, w_hbm,
    xo_ref, go_ref, sum_ref, upo_ref, tot_ref,
    x_v, gate_v, up_v, hid_v, seg_ref, dw_ref, w_v, x32, g32, part, cnt,
    xp, xq, gr, rs1, rs2, rs3, cntr, lsem, ssem, rsem,
):
    r, s = lax.axis_index("replica"), lax.axis_index("shard")
    core, side, across = flip(r, 1), flip(r, 2), flip(flip(r, 1), 2)
    near, mid, far = flip(s, 1), flip(s, 2), flip(s, 4)
    rows, width = x_v.shape[0], xo_ref.shape[1]
    quarter = rows // QUARTERS
    tall = sum_ref.shape[0]
    f32, bf16 = jnp.float32, jnp.bfloat16

    local = []
    for k, (src, dst) in enumerate(
        [
            (x_hbm, x_v), (seg_hbm, seg_ref), (dw_hbm, dw_ref), (gate_hbm, gate_v),
            (hid_hbm, hid_v), (up_hbm, up_v), (w_hbm, w_v),
        ]
    ):
        copy = pltpu.make_async_copy(src, dst, lsem.at[k])
        copy.start()
        local.append(copy)

    barrier = pltpu.get_barrier_semaphore()
    peers = [(core, s), (side, s), (across, s), (r, near), (r, mid), (r, far)]
    for peer in peers:
        pl.semaphore_signal(barrier, inc=1, device_id=peer, device_id_type=MESH)

    started = []

    def push(src, dst, peer):
        k = len(started)
        copy = pltpu.make_async_remote_copy(
            src_ref=src, dst_ref=dst, send_sem=ssem.at[k], recv_sem=rsem.at[k],
            device_id=peer, device_id_type=MESH,
        )
        copy.start()
        started.append(copy)
        return copy

    local[0].wait()
    x32[...] = x_v[...].astype(f32)
    own = pl.ds(pl.multiple_of(r * width, width), width)
    xo_ref[pl.ds(0, rows), :] = x_v[:, own]

    local[1].wait()
    local[2].wait()
    docs = dw_ref.shape[1]
    seg = jnp.broadcast_to(seg_ref[...].astype(f32), (128, rows)).T[:, :docs]
    labels = lax.broadcasted_iota(jnp.int32, (rows, docs), 1).astype(f32)
    dw = jnp.broadcast_to(dw_ref[...].astype(f32), (rows, docs))
    tw = jnp.sum(jnp.where(seg == labels, dw, 0.0), axis=1, keepdims=True)
    count = jnp.sum(tw, axis=0, keepdims=True)
    cnt[...] = jnp.broadcast_to(count, cnt.shape)

    pl.semaphore_wait(barrier, len(peers))

    q = lax.rem(s, QUARTERS)

    def at_quarter(index):
        return pl.ds(pl.multiple_of(index * quarter, quarter), quarter)

    def columns(owner):
        return pl.ds(pl.multiple_of(owner * width, width), width)

    x_side = push(x32.at[at_quarter(q), columns(side)], xq.at[0, 0], (side, s))
    x_across = push(x32.at[at_quarter(q), columns(across)], xq.at[1, 0], (across, s))
    x_core = push(x32.at[:, columns(core)], xp, (core, s))
    counts = [push(cnt, cntr.at[k], (peer, s)) for k, peer in enumerate((core, side, across))]

    for k in (3, 4, 5):
        local[k].wait()
    for k in range(QUARTERS):
        at = pl.ds(k * quarter, quarter)
        g = gate_v[at, :].astype(f32)
        sig = jax.nn.sigmoid(g)
        h = hid_v[at, :].astype(f32) * tw[k * quarter : (k + 1) * quarter, :]
        raw = (h * up_v[at, :].astype(f32) * sig * (1.0 + g * (1.0 - sig))).astype(bf16)
        upo_ref[at, :] = h * g * sig
        go_ref[at, :] = raw
        g32[at, :] = raw.astype(f32)

    g_side = [
        push(g32.at[pl.ds(k * quarter, quarter), :], gr.at[1, pl.ds(k * quarter, quarter), :], (side, s))
        for k in range(QUARTERS)
    ]
    g_core = push(g32, gr.at[0], (core, s))

    local[6].wait()
    step = w_v.shape[0] // QUARTERS
    for k in range(QUARTERS):
        part[:, pl.ds(k * step, step)] = lax.dot_general(
            go_ref[pl.ds(0, rows), :], w_v[pl.ds(k * step, step), :],
            (((1,), (1,)), ((), ())), preferred_element_type=f32,
        )

    def block(index):
        return pl.ds(pl.multiple_of(index * tall, tall), tall)

    first = {}
    for slot, (delta, index) in enumerate(
        [(6, flip(flip(near, 2), 4)), (2, flip(near, 2)), (4, flip(near, 4)), (0, near)]
    ):
        first[delta] = (slot, push(part.at[block(index), :], rs1.at[slot], (r, near)))

    def absorb(delta, index):
        slot, copy = first[delta]
        copy.wait_recv()
        part[block(index), :] = part[block(index), :] + rs1[slot]

    def keep_x(group, slot, index):
        xo_ref[pl.ds(pl.multiple_of((group + 2) * rows + index * quarter, quarter), quarter), :] = (
            xq[group, slot].astype(bf16)
        )

    def keep_g(group, k):
        at = pl.ds(k * quarter, quarter)
        go_ref[pl.ds((group + 1) * rows + k * quarter, quarter), :] = gr[group, at, :].astype(bf16)

    def relay_g(k):
        at = pl.ds(k * quarter, quarter)
        g_side[k].wait_recv()
        copy = push(gr.at[1, at, :], gr.at[2, at, :], (core, s))
        keep_g(1, k)
        return copy

    x_near, x_mid = [], []
    for group, copy in enumerate((x_side, x_across)):
        copy.wait_recv()
        x_near.append(push(xq.at[group, 0], xq.at[group, 1], (r, near)))
        x_mid.append(push(xq.at[group, 0], xq.at[group, 2], (r, mid)))
    x_core.wait_recv()
    xo_ref[pl.ds(rows, rows), :] = xp[...].astype(bf16)
    g_core.wait_recv()
    for k in range(QUARTERS):
        keep_g(0, k)
    for group in range(2):
        keep_x(group, 0, q)
    for copy in counts:
        copy.wait_recv()
    tot_ref[...] = cnt[...] + cntr[0] + cntr[1] + cntr[2]

    g_across = [relay_g(0)]
    absorb(6, flip(mid, 4))
    second_far = push(part.at[block(flip(mid, 4)), :], rs2.at[0], (r, mid))
    absorb(2, mid)
    second_own = push(part.at[block(mid), :], rs2.at[1], (r, mid))
    g_across.append(relay_g(1))
    absorb(4, far)
    second_far.wait_recv()
    part[block(far), :] = part[block(far), :] + rs2[0]
    third = push(part.at[block(far), :], rs3, (r, far))
    x_last = []
    for group in range(2):
        x_near[group].wait_recv()
        x_last.append(push(xq.at[group, 1], xq.at[group, 3], (r, mid)))
        keep_x(group, 1, lax.rem(near, QUARTERS))
    g_across.append(relay_g(2))
    for group in range(2):
        x_mid[group].wait_recv()
        keep_x(group, 2, lax.rem(mid, QUARTERS))
    for k in range(2):
        g_across[k].wait_recv()
        keep_g(2, k)
    absorb(0, s)
    second_own.wait_recv()
    g_across.append(relay_g(3))
    for group in range(2):
        x_last[group].wait_recv()
        keep_x(group, 3, lax.rem(flip(near, 2), QUARTERS))
    third.wait_recv()
    sum_ref[...] = part[block(s), :] + rs2[1] + rs3[...]
    for k in range(2, QUARTERS):
        g_across[k].wait_recv()
        keep_g(2, k)
    for copy in started:
        copy.wait_send()


def exchange(inputs, gate_pre, up_pre, hidden_grad, segment_ids, doc_weight, w_gate):
    replicas, shards = lax.axis_size("replica"), lax.axis_size("shard")
    rows, features = inputs.shape
    hidden = gate_pre.shape[1]
    width, tall, quarter = features // replicas, rows // shards, rows // QUARTERS
    f32, bf16 = jnp.float32, jnp.bfloat16
    vmem = pl.BlockSpec(memory_space=pltpu.VMEM)
    hbm = pl.BlockSpec(memory_space=pltpu.HBM)
    copies = 30
    return pl.pallas_call(
        exchange_kernel,
        out_shape=(
            jax.ShapeDtypeStruct((replicas * rows, width), bf16),
            jax.ShapeDtypeStruct((replicas * rows, hidden), bf16),
            jax.ShapeDtypeStruct((tall, features), f32),
            jax.ShapeDtypeStruct((rows, hidden), f32),
            jax.ShapeDtypeStruct((8, 128), f32),
        ),
        in_specs=[hbm] * 7,
        out_specs=(vmem,) * 5,
        scratch_shapes=[
            pltpu.VMEM((rows, features), bf16),
            pltpu.VMEM((rows, hidden), bf16),
            pltpu.VMEM((rows, hidden), bf16),
            pltpu.VMEM((rows, hidden), bf16),
            pltpu.VMEM(segment_ids.shape, jnp.int32),
            pltpu.VMEM(doc_weight.shape, jnp.int32),
            pltpu.VMEM((features, hidden), bf16),
            pltpu.VMEM((rows, features), f32),
            pltpu.VMEM((rows, hidden), f32),
            pltpu.VMEM((rows, features), f32),
            pltpu.VMEM((8, 128), f32),
            pltpu.VMEM((rows, width), f32),
            pltpu.VMEM((2, QUARTERS, quarter, width), f32),
            pltpu.VMEM((3, rows, hidden), f32),
            pltpu.VMEM((4, tall, features), f32),
            pltpu.VMEM((2, tall, features), f32),
            pltpu.VMEM((tall, features), f32),
            pltpu.VMEM((3, 8, 128), f32),
            pltpu.SemaphoreType.DMA((7,)),
            pltpu.SemaphoreType.DMA((copies,)),
            pltpu.SemaphoreType.DMA((copies,)),
        ],
        compiler_params=pltpu.CompilerParams(
            collective_id=0, has_side_effects=True, vmem_limit_bytes=24 * 1024 * 1024
        ),
        cost_estimate=pl.CostEstimate(
            flops=2 * rows * hidden * features, bytes_accessed=40 * 1024 * 1024, transcendentals=0
        ),
        name="exchange",
    )(inputs, gate_pre, up_pre, hidden_grad, segment_ids, doc_weight, w_gate)


def gather_path(
    inputs, gate_pre, up_pre, hidden_grad, segment_ids, doc_weight, w_gate, master, moment, second
):
    group_rows = inputs.shape[0]
    replicas = lax.axis_size("replica")
    x_all, gate_all, input_summed, up_part, totals = exchange(
        inputs, gate_pre, up_pre, hidden_grad, segment_ids, doc_weight, w_gate
    )
    total = totals[0, 0]
    scale = jnp.float32(group_rows * replicas) / total
    group_scale = jnp.float32(group_rows) / total
    input_grad = (input_summed * scale).astype(jnp.bfloat16)
    up_grad = (up_part * scale).astype(jnp.bfloat16)
    summed_grad = lax.dot_general(
        x_all, gate_all, (((0,), (0,)), ((), ())), preferred_element_type=jnp.float32
    )
    return (input_grad, up_grad) + adamw(summed_grad * group_scale, master, moment, second)


def on_device(*args):
    inputs, gate_pre = args[:2]
    replicas, shards = lax.axis_size("replica"), lax.axis_size("shard")
    rows, features = inputs.shape
    hidden = gate_pre.shape[1]
    gathered = replicas * rows * (features // replicas + hidden)
    fits = rows % (QUARTERS * 32) == 0 and features % (replicas * 128) == 0
    if (replicas, shards) == (4, 8) and fits and gathered <= features * hidden:
        return gather_path(*args)
    return reduce_path(*args)


def solution(mesh):
    in_specs = (
        P("replica", None),
        P("replica", "shard"),
        P("replica", "shard"),
        P("replica", "shard"),
        P("replica", None),
        P("replica", None),
        P(None, "shard"),
        P("replica", "shard"),
        P("replica", "shard"),
        P("replica", "shard"),
    )
    out_specs = (
        P(("replica", "shard"), None),
        P("replica", "shard"),
        P("replica", "shard"),
        P("replica", "shard"),
        P("replica", "shard"),
    )
    return jax.shard_map(
        on_device, mesh=mesh, in_specs=in_specs, out_specs=out_specs, check_vma=False
    )
```

```python
import functools

import jax
import jax.numpy as jnp
from jax import lax
from jax.experimental import pallas as pl
from jax.experimental.pallas import tpu as pltpu
from jax.sharding import PartitionSpec as P

MESH = pl.DeviceIdType.MESH
QUARTERS = 4


def token_weights(segment_ids, doc_weight):
    labels = jnp.arange(doc_weight.shape[1], dtype=jnp.int32)
    onehot = segment_ids[:, :, None] == labels[None, None, :]
    return jnp.sum(jnp.where(onehot, doc_weight[:, None, :], 0), axis=2)


def adamw(grad, master, moment, second):
    moment_new = 0.9 * moment + 0.1 * grad
    second_new = 0.95 * second + 0.05 * grad * grad
    first_fix = moment_new / (1.0 - 0.9**8)
    second_fix = second_new / (1.0 - 0.95**8)
    master_new = master - 0.003 * (first_fix / (jnp.sqrt(second_fix) + 1e-08) + 0.1 * master)
    return master_new, moment_new, second_new


def reduce_path(
    inputs, gate_pre, up_pre, hidden_grad, segment_ids, doc_weight, w_gate, master, moment, second
):
    group_rows = inputs.shape[0]
    replicas = lax.axis_size("replica")
    weights = token_weights(segment_ids, doc_weight)[0]
    local_count = jnp.sum(weights)
    gate_f = gate_pre.astype(jnp.float32)
    sigmoid_gate = jax.nn.sigmoid(gate_f)
    weighted = hidden_grad.astype(jnp.float32) * weights.astype(jnp.float32)[:, None]
    gate_raw = (
        weighted * up_pre.astype(jnp.float32) * sigmoid_gate * (1.0 + gate_f * (1.0 - sigmoid_gate))
    ).astype(jnp.bfloat16)
    up_part = weighted * gate_f * sigmoid_gate
    input_part = lax.dot_general(
        gate_raw, w_gate, (((1,), (1,)), ((), ())), preferred_element_type=jnp.float32
    )
    input_summed = lax.psum_scatter(input_part, "shard", scatter_dimension=0, tiled=True)
    total = lax.psum(local_count, "replica").astype(jnp.float32)
    summed_grad = lax.psum_scatter(
        lax.dot_general(
            inputs, gate_raw, (((0,), (0,)), ((), ())), preferred_element_type=jnp.float32
        ),
        "replica",
        scatter_dimension=0,
        tiled=True,
    )
    scale = jnp.float32(group_rows * replicas) / total
    group_scale = jnp.float32(group_rows) / total
    input_grad = (input_summed * scale).astype(jnp.bfloat16)
    up_grad = (up_part * scale).astype(jnp.bfloat16)
    return (input_grad, up_grad) + adamw(summed_grad * group_scale, master, moment, second)


def flip(index, bit):
    return index + bit - 2 * bit * lax.rem(lax.div(index, bit), 2)


def exchange_kernel(
    x_hbm, gate_hbm, up_hbm, hid_hbm, seg_hbm, dw_hbm, w_hbm,
    xo_hbm, go_hbm, sum_hbm, upo_hbm, gs_hbm,
    xo_ref, go_ref, sum_ref, upo_ref, gs_ref, x_v, gate_v, up_v, hid_v, seg_ref, dw_ref, w_v, x32, g32, part, cnt,
    xp, xq, gr, rs1, rs2, rs3, cntr, lsem, osem, ssem, rsem,
):
    r, s = lax.axis_index("replica"), lax.axis_index("shard")
    replicas = lax.axis_size("replica")
    core, side, across = flip(r, 1), flip(r, 2), flip(flip(r, 1), 2)
    near, mid, far = flip(s, 1), flip(s, 2), flip(s, 4)
    rows, width = x_v.shape[0], xo_ref.shape[1]
    quarter = rows // QUARTERS
    tall = sum_ref.shape[0]
    f32, bf16 = jnp.float32, jnp.bfloat16

    local = []
    for k, (src, dst) in enumerate(
        [
            (x_hbm, x_v), (seg_hbm, seg_ref), (dw_hbm, dw_ref), (gate_hbm, gate_v),
            (hid_hbm, hid_v), (up_hbm, up_v), (w_hbm, w_v),
        ]
    ):
        copy = pltpu.make_async_copy(src, dst, lsem.at[k])
        copy.start()
        local.append(copy)

    barrier = pltpu.get_barrier_semaphore()
    peers = [(core, s), (side, s), (across, s), (r, near), (r, mid), (r, far)]
    for peer in peers:
        pl.semaphore_signal(barrier, inc=1, device_id=peer, device_id_type=MESH)

    started, written = [], []

    def write(src, dst):
        copy = pltpu.make_async_copy(src, dst, osem.at[len(written)])
        copy.start()
        written.append(copy)

    def push(src, dst, peer):
        k = len(started)
        copy = pltpu.make_async_remote_copy(
            src_ref=src, dst_ref=dst, send_sem=ssem.at[k], recv_sem=rsem.at[k],
            device_id=peer, device_id_type=MESH,
        )
        copy.start()
        started.append(copy)
        return copy

    local[0].wait()
    x32[...] = x_v[...].astype(f32)
    own = pl.ds(pl.multiple_of(r * width, width), width)
    xo_ref[pl.ds(0, rows), :] = x_v[:, own]

    local[1].wait()
    local[2].wait()
    docs = dw_ref.shape[1]
    seg = jnp.broadcast_to(seg_ref[...].astype(f32), (128, rows)).T[:, :docs]
    labels = lax.broadcasted_iota(jnp.int32, (rows, docs), 1).astype(f32)
    dw = jnp.broadcast_to(dw_ref[...].astype(f32), (rows, docs))
    tw = jnp.sum(jnp.where(seg == labels, dw, 0.0), axis=1, keepdims=True)
    count = jnp.sum(tw, axis=0, keepdims=True)
    cnt[...] = jnp.broadcast_to(count, cnt.shape)

    pl.semaphore_wait(barrier, len(peers))

    q = lax.rem(s, QUARTERS)

    def at_quarter(index):
        return pl.ds(pl.multiple_of(index * quarter, quarter), quarter)

    def columns(owner):
        return pl.ds(pl.multiple_of(owner * width, width), width)

    x_side = push(x32.at[at_quarter(q), columns(side)], xq.at[0, 0], (side, s))
    x_across = push(x32.at[at_quarter(q), columns(across)], xq.at[1, 0], (across, s))
    x_core = push(x32.at[:, columns(core)], xp, (core, s))
    counts = [push(cnt, cntr.at[k], (peer, s)) for k, peer in enumerate((core, side, across))]

    for k in (3, 4, 5):
        local[k].wait()
    for k in range(QUARTERS):
        at = pl.ds(k * quarter, quarter)
        g = gate_v[at, :].astype(f32)
        sig = jax.nn.sigmoid(g)
        h = hid_v[at, :].astype(f32) * tw[k * quarter : (k + 1) * quarter, :]
        raw = (h * up_v[at, :].astype(f32) * sig * (1.0 + g * (1.0 - sig))).astype(bf16)
        upo_ref[at, :] = h * g * sig
        go_ref[at, :] = raw
        g32[at, :] = raw.astype(f32)

    g_side = [
        push(g32.at[pl.ds(k * quarter, quarter), :], gr.at[1, pl.ds(k * quarter, quarter), :], (side, s))
        for k in range(QUARTERS)
    ]
    g_core = push(g32, gr.at[0], (core, s))

    local[6].wait()
    step = w_v.shape[0] // QUARTERS
    for k in range(QUARTERS):
        part[:, pl.ds(k * step, step)] = lax.dot_general(
            go_ref[pl.ds(0, rows), :], w_v[pl.ds(k * step, step), :],
            (((1,), (1,)), ((), ())), preferred_element_type=f32,
        )

    def block(index):
        return pl.ds(pl.multiple_of(index * tall, tall), tall)

    first = {}
    for slot, (delta, index) in enumerate(
        [(6, flip(flip(near, 2), 4)), (2, flip(near, 2)), (4, flip(near, 4)), (0, near)]
    ):
        first[delta] = (slot, push(part.at[block(index), :], rs1.at[slot], (r, near)))

    def absorb(delta, index):
        slot, copy = first[delta]
        copy.wait_recv()
        part[block(index), :] = part[block(index), :] + rs1[slot]

    def keep_x(group, slot, index):
        xo_ref[pl.ds(pl.multiple_of((group + 2) * rows + index * quarter, quarter), quarter), :] = (
            xq[group, slot].astype(bf16)
        )

    def keep_g(group, k):
        at = pl.ds(k * quarter, quarter)
        go_ref[pl.ds((group + 1) * rows + k * quarter, quarter), :] = gr[group, at, :].astype(bf16)

    def relay_g(k):
        at = pl.ds(k * quarter, quarter)
        g_side[k].wait_recv()
        copy = push(gr.at[1, at, :], gr.at[2, at, :], (core, s))
        keep_g(1, k)
        return copy

    x_near, x_mid = [], []
    for group, copy in enumerate((x_side, x_across)):
        copy.wait_recv()
        x_near.append(push(xq.at[group, 0], xq.at[group, 1], (r, near)))
        x_mid.append(push(xq.at[group, 0], xq.at[group, 2], (r, mid)))
    x_core.wait_recv()
    xo_ref[pl.ds(rows, rows), :] = xp[...].astype(bf16)
    g_core.wait_recv()
    for k in range(QUARTERS):
        keep_g(0, k)
    for group in range(2):
        keep_x(group, 0, q)
    for copy in counts:
        copy.wait_recv()
    total = (cnt[...] + cntr[0] + cntr[1] + cntr[2])[0:1, 0:1]
    scale = f32(rows * replicas) / total
    gs_ref[...] = jnp.broadcast_to(f32(rows) / total, gs_ref.shape)
    upo_ref[...] = upo_ref[...] * scale
    write(xo_ref.at[pl.ds(0, 2 * rows), :], xo_hbm.at[pl.ds(0, 2 * rows), :])
    write(go_ref.at[pl.ds(0, 2 * rows), :], go_hbm.at[pl.ds(0, 2 * rows), :])
    write(gs_ref, gs_hbm)
    write(upo_ref, upo_hbm)

    g_across = [relay_g(0)]
    absorb(6, flip(mid, 4))
    second_far = push(part.at[block(flip(mid, 4)), :], rs2.at[0], (r, mid))
    absorb(2, mid)
    second_own = push(part.at[block(mid), :], rs2.at[1], (r, mid))
    g_across.append(relay_g(1))
    absorb(4, far)
    second_far.wait_recv()
    part[block(far), :] = part[block(far), :] + rs2[0]
    third = push(part.at[block(far), :], rs3, (r, far))
    x_last = []
    for group in range(2):
        x_near[group].wait_recv()
        x_last.append(push(xq.at[group, 1], xq.at[group, 3], (r, mid)))
        keep_x(group, 1, lax.rem(near, QUARTERS))
    g_across.append(relay_g(2))
    for group in range(2):
        x_mid[group].wait_recv()
        keep_x(group, 2, lax.rem(mid, QUARTERS))
    for k in range(2):
        g_across[k].wait_recv()
        keep_g(2, k)
    absorb(0, s)
    second_own.wait_recv()
    g_across.append(relay_g(3))
    for group in range(2):
        x_last[group].wait_recv()
        keep_x(group, 3, lax.rem(flip(near, 2), QUARTERS))
    write(xo_ref.at[pl.ds(2 * rows, 2 * rows), :], xo_hbm.at[pl.ds(2 * rows, 2 * rows), :])
    write(go_ref.at[pl.ds(2 * rows, rows), :], go_hbm.at[pl.ds(2 * rows, rows), :])
    third.wait_recv()
    sum_ref[...] = (part[block(s), :] + rs2[1] + rs3[...]) * scale
    write(sum_ref, sum_hbm)
    for k in range(2, QUARTERS):
        g_across[k].wait_recv()
        keep_g(2, k)
    write(go_ref.at[pl.ds(3 * rows, rows), :], go_hbm.at[pl.ds(3 * rows, rows), :])
    for copy in started:
        copy.wait_send()
    for copy in written:
        copy.wait()


def exchange(inputs, gate_pre, up_pre, hidden_grad, segment_ids, doc_weight, w_gate):
    replicas, shards = lax.axis_size("replica"), lax.axis_size("shard")
    rows, features = inputs.shape
    hidden = gate_pre.shape[1]
    width, tall, quarter = features // replicas, rows // shards, rows // QUARTERS
    f32, bf16 = jnp.float32, jnp.bfloat16
    hbm = pl.BlockSpec(memory_space=pltpu.HBM)
    copies = 30
    return pl.pallas_call(
        exchange_kernel,
        out_shape=(
            jax.ShapeDtypeStruct((replicas * rows, width), bf16),
            jax.ShapeDtypeStruct((replicas * rows, hidden), bf16),
            jax.ShapeDtypeStruct((tall, features), f32),
            jax.ShapeDtypeStruct((rows, hidden), f32),
            jax.ShapeDtypeStruct((8, hidden), f32),
        ),
        in_specs=[hbm] * 7,
        out_specs=(hbm,) * 5,
        scratch_shapes=[
            pltpu.VMEM((replicas * rows, width), bf16),
            pltpu.VMEM((replicas * rows, hidden), bf16),
            pltpu.VMEM((tall, features), f32),
            pltpu.VMEM((rows, hidden), f32),
            pltpu.VMEM((8, hidden), f32),
            pltpu.VMEM((rows, features), bf16),
            pltpu.VMEM((rows, hidden), bf16),
            pltpu.VMEM((rows, hidden), bf16),
            pltpu.VMEM((rows, hidden), bf16),
            pltpu.VMEM(segment_ids.shape, jnp.int32),
            pltpu.VMEM(doc_weight.shape, jnp.int32),
            pltpu.VMEM((features, hidden), bf16),
            pltpu.VMEM((rows, features), f32),
            pltpu.VMEM((rows, hidden), f32),
            pltpu.VMEM((rows, features), f32),
            pltpu.VMEM((8, 128), f32),
            pltpu.VMEM((rows, width), f32),
            pltpu.VMEM((2, QUARTERS, quarter, width), f32),
            pltpu.VMEM((3, rows, hidden), f32),
            pltpu.VMEM((4, tall, features), f32),
            pltpu.VMEM((2, tall, features), f32),
            pltpu.VMEM((tall, features), f32),
            pltpu.VMEM((3, 8, 128), f32),
            pltpu.SemaphoreType.DMA((7,)),
            pltpu.SemaphoreType.DMA((8,)),
            pltpu.SemaphoreType.DMA((copies,)),
            pltpu.SemaphoreType.DMA((copies,)),
        ],
        compiler_params=pltpu.CompilerParams(
            collective_id=0, has_side_effects=True, vmem_limit_bytes=54 * 1024 * 1024
        ),
        cost_estimate=pl.CostEstimate(
            flops=2 * rows * hidden * features, bytes_accessed=40 * 1024 * 1024, transcendentals=0
        ),
        name="exchange",
    )(inputs, gate_pre, up_pre, hidden_grad, segment_ids, doc_weight, w_gate)


def step_kernel(
    x_hbm, g_hbm, sum_hbm, up_hbm, gs_hbm, ma_old, mo_old, se_old,
    ig_hbm, ug_hbm, ma_hbm, mo_hbm, se_hbm,
    x_ref, g_ref, sum_ref, up_ref, gs_ref, ma_ref, mo_ref, se_ref, ig_v, ug_v, ma_v, mo_v, se_v, isem, sems,
):
    band = ma_v.shape[1]
    written, loaded = [], []
    bands = [pl.ds(k * band, band) for k in range(ma_v.shape[0])]
    loads = [(g_hbm, g_ref), (x_hbm, x_ref), (gs_hbm, gs_ref)]
    for at in bands:
        loads += [
            (old.at[at, :], new.at[at, :])
            for old, new in ((mo_old, mo_ref), (se_old, se_ref), (ma_old, ma_ref))
        ]
    for k, (src, dst) in enumerate(loads + [(sum_hbm, sum_ref), (up_hbm, up_ref)]):
        copy = pltpu.make_async_copy(src, dst, isem.at[k])
        copy.start()
        loaded.append(copy)

    def write(src, dst):
        copy = pltpu.make_async_copy(src, dst, sems.at[len(written)])
        copy.start()
        written.append(copy)

    for copy in loaded[:3]:
        copy.wait()
    group_scale = gs_ref[0:1, :]
    for k, at in enumerate(bands):
        raw = lax.dot_general(
            x_ref[:, at], g_ref[...], (((0,), (0,)), ((), ())), preferred_element_type=jnp.float32
        )
        grad = raw * group_scale
        for copy in loaded[3 + 3 * k : 6 + 3 * k]:
            copy.wait()
        moment_new = 0.9 * mo_ref[at, :] + 0.1 * grad
        second_new = 0.95 * se_ref[at, :] + 0.05 * grad * grad
        mo_v[k] = moment_new
        se_v[k] = second_new
        master = ma_ref[at, :]
        first_fix = moment_new * (1.0 / (1.0 - 0.9**8))
        second_fix = second_new * (1.0 / (1.0 - 0.95**8))
        ma_v[k] = master - 0.003 * (first_fix / (jnp.sqrt(second_fix) + 1e-08) + 0.1 * master)
        write(mo_v.at[k], mo_hbm.at[at, :])
        write(se_v.at[k], se_hbm.at[at, :])
        write(ma_v.at[k], ma_hbm.at[at, :])
    for copy in loaded[3 + 3 * len(bands) :]:
        copy.wait()
    ig_v[...] = sum_ref[...].astype(ig_v.dtype)
    ug_v[...] = up_ref[...].astype(ug_v.dtype)
    write(ig_v, ig_hbm)
    write(ug_v, ug_hbm)
    for copy in written:
        copy.wait()


def step(x_all, gate_all, input_scaled, up_scaled, group_scale, master, moment, second):
    states = master.shape
    bands = 4
    f32, bf16 = jnp.float32, jnp.bfloat16
    hbm = pl.BlockSpec(memory_space=pltpu.HBM)
    banded = pltpu.VMEM((bands, states[0] // bands, states[1]), f32)
    return pl.pallas_call(
        step_kernel,
        out_shape=(
            jax.ShapeDtypeStruct(input_scaled.shape, bf16),
            jax.ShapeDtypeStruct(up_scaled.shape, bf16),
        )
        + (jax.ShapeDtypeStruct(states, f32),) * 3,
        in_specs=[hbm] * 8,
        out_specs=(hbm,) * 5,
        scratch_shapes=[
            pltpu.VMEM(x_all.shape, bf16),
            pltpu.VMEM(gate_all.shape, bf16),
            pltpu.VMEM(input_scaled.shape, f32),
            pltpu.VMEM(up_scaled.shape, f32),
            pltpu.VMEM(group_scale.shape, f32),
            pltpu.VMEM(states, f32),
            pltpu.VMEM(states, f32),
            pltpu.VMEM(states, f32),
            pltpu.VMEM(input_scaled.shape, bf16),
            pltpu.VMEM(up_scaled.shape, bf16),
            banded,
            banded,
            banded,
            pltpu.SemaphoreType.DMA((5 + 3 * bands,)),
            pltpu.SemaphoreType.DMA((2 + 3 * bands,)),
        ],
        compiler_params=pltpu.CompilerParams(vmem_limit_bytes=54 * 1024 * 1024),
        name="step",
    )(x_all, gate_all, input_scaled, up_scaled, group_scale, master, moment, second)


def gather_path(
    inputs, gate_pre, up_pre, hidden_grad, segment_ids, doc_weight, w_gate, master, moment, second
):
    factors = exchange(inputs, gate_pre, up_pre, hidden_grad, segment_ids, doc_weight, w_gate)
    return step(*factors, master, moment, second)


def on_device(*args):
    inputs, gate_pre = args[:2]
    replicas, shards = lax.axis_size("replica"), lax.axis_size("shard")
    rows, features = inputs.shape
    hidden = gate_pre.shape[1]
    gathered = replicas * rows * (features // replicas + hidden)
    fits = rows % (QUARTERS * 32) == 0 and features % (replicas * 128) == 0
    if (replicas, shards) == (4, 8) and fits and gathered <= features * hidden:
        return gather_path(*args)
    return reduce_path(*args)


def solution(mesh):
    in_specs = (
        P("replica", None),
        P("replica", "shard"),
        P("replica", "shard"),
        P("replica", "shard"),
        P("replica", None),
        P("replica", None),
        P(None, "shard"),
        P("replica", "shard"),
        P("replica", "shard"),
        P("replica", "shard"),
    )
    out_specs = (
        P(("replica", "shard"), None),
        P("replica", "shard"),
        P("replica", "shard"),
        P("replica", "shard"),
        P("replica", "shard"),
    )
    return jax.shard_map(
        on_device, mesh=mesh, in_specs=in_specs, out_specs=out_specs, check_vma=False
    )
```

```python
import functools

import jax
import jax.numpy as jnp
from jax import lax
from jax.experimental import pallas as pl
from jax.experimental.pallas import tpu as pltpu
from jax.sharding import PartitionSpec as P

MESH = pl.DeviceIdType.MESH
QUARTERS = 4


def token_weights(segment_ids, doc_weight):
    labels = jnp.arange(doc_weight.shape[1], dtype=jnp.int32)
    onehot = segment_ids[:, :, None] == labels[None, None, :]
    return jnp.sum(jnp.where(onehot, doc_weight[:, None, :], 0), axis=2)


def adamw(grad, master, moment, second):
    moment_new = 0.9 * moment + 0.1 * grad
    second_new = 0.95 * second + 0.05 * grad * grad
    first_fix = moment_new / (1.0 - 0.9**8)
    second_fix = second_new / (1.0 - 0.95**8)
    master_new = master - 0.003 * (first_fix / (jnp.sqrt(second_fix) + 1e-08) + 0.1 * master)
    return master_new, moment_new, second_new


def reduce_path(
    inputs, gate_pre, up_pre, hidden_grad, segment_ids, doc_weight, w_gate, master, moment, second
):
    group_rows = inputs.shape[0]
    replicas = lax.axis_size("replica")
    weights = token_weights(segment_ids, doc_weight)[0]
    local_count = jnp.sum(weights)
    gate_f = gate_pre.astype(jnp.float32)
    sigmoid_gate = jax.nn.sigmoid(gate_f)
    weighted = hidden_grad.astype(jnp.float32) * weights.astype(jnp.float32)[:, None]
    gate_raw = (
        weighted * up_pre.astype(jnp.float32) * sigmoid_gate * (1.0 + gate_f * (1.0 - sigmoid_gate))
    ).astype(jnp.bfloat16)
    up_part = weighted * gate_f * sigmoid_gate
    input_part = lax.dot_general(
        gate_raw, w_gate, (((1,), (1,)), ((), ())), preferred_element_type=jnp.float32
    )
    input_summed = lax.psum_scatter(input_part, "shard", scatter_dimension=0, tiled=True)
    total = lax.psum(local_count, "replica").astype(jnp.float32)
    summed_grad = lax.psum_scatter(
        lax.dot_general(
            inputs, gate_raw, (((0,), (0,)), ((), ())), preferred_element_type=jnp.float32
        ),
        "replica",
        scatter_dimension=0,
        tiled=True,
    )
    scale = jnp.float32(group_rows * replicas) / total
    group_scale = jnp.float32(group_rows) / total
    input_grad = (input_summed * scale).astype(jnp.bfloat16)
    up_grad = (up_part * scale).astype(jnp.bfloat16)
    return (input_grad, up_grad) + adamw(summed_grad * group_scale, master, moment, second)


def flip(index, bit):
    return index + bit - 2 * bit * lax.rem(lax.div(index, bit), 2)


def exchange_kernel(
    x_hbm, gate_hbm, up_hbm, hid_hbm, seg_hbm, dw_hbm, w_hbm,
    xo_hbm, go_hbm, sum_hbm, upo_hbm, gs_hbm,
    xo_ref, go_ref, sum_ref, upo_ref, gs_ref, x_v, gate_v, up_v, hid_v, seg_ref, dw_ref, w_v, x32, g32, part, cnt,
    xp, xq, gr, rs1, rs2, rs3, cntr, lsem, osem, ssem, rsem,
):
    r, s = lax.axis_index("replica"), lax.axis_index("shard")
    replicas = lax.axis_size("replica")
    core, side, across = flip(r, 1), flip(r, 2), flip(flip(r, 1), 2)
    near, mid, far = flip(s, 1), flip(s, 2), flip(s, 4)
    rows, width = x_v.shape[0], xo_ref.shape[1]
    quarter = rows // QUARTERS
    tall = sum_ref.shape[0]
    f32, bf16 = jnp.float32, jnp.bfloat16

    local = []
    for k, (src, dst) in enumerate(
        [
            (x_hbm, x_v), (seg_hbm, seg_ref), (dw_hbm, dw_ref), (gate_hbm, gate_v),
            (hid_hbm, hid_v), (up_hbm, up_v), (w_hbm, w_v),
        ]
    ):
        copy = pltpu.make_async_copy(src, dst, lsem.at[k])
        copy.start()
        local.append(copy)

    barrier = pltpu.get_barrier_semaphore()
    peers = [(core, s), (side, s), (across, s), (r, near), (r, mid), (r, far)]
    for peer in peers:
        pl.semaphore_signal(barrier, inc=1, device_id=peer, device_id_type=MESH)

    started, written = [], []

    def write(src, dst):
        copy = pltpu.make_async_copy(src, dst, osem.at[len(written)])
        copy.start()
        written.append(copy)

    def push(src, dst, peer):
        k = len(started)
        copy = pltpu.make_async_remote_copy(
            src_ref=src, dst_ref=dst, send_sem=ssem.at[k], recv_sem=rsem.at[k],
            device_id=peer, device_id_type=MESH,
        )
        copy.start()
        started.append(copy)
        return copy

    local[0].wait()
    x32[...] = x_v[...].astype(f32)
    own = pl.ds(pl.multiple_of(r * width, width), width)
    xo_ref[pl.ds(0, rows), :] = x_v[:, own]

    local[1].wait()
    local[2].wait()
    docs = dw_ref.shape[1]
    seg = jnp.broadcast_to(seg_ref[...].astype(f32), (128, rows)).T[:, :docs]
    labels = lax.broadcasted_iota(jnp.int32, (rows, docs), 1).astype(f32)
    dw = jnp.broadcast_to(dw_ref[...].astype(f32), (rows, docs))
    tw = jnp.sum(jnp.where(seg == labels, dw, 0.0), axis=1, keepdims=True)
    count = jnp.sum(tw, axis=0, keepdims=True)
    cnt[...] = jnp.broadcast_to(count, cnt.shape)

    pl.semaphore_wait(barrier, len(peers))

    q = lax.rem(s, QUARTERS)

    def at_quarter(index):
        return pl.ds(pl.multiple_of(index * quarter, quarter), quarter)

    def columns(owner):
        return pl.ds(pl.multiple_of(owner * width, width), width)

    x_side = push(x32.at[at_quarter(q), columns(side)], xq.at[0, 0], (side, s))
    x_across = push(x32.at[at_quarter(q), columns(across)], xq.at[1, 0], (across, s))
    x_core = push(x32.at[:, columns(core)], xp, (core, s))
    counts = [push(cnt, cntr.at[k], (peer, s)) for k, peer in enumerate((core, side, across))]

    for k in (3, 4, 5):
        local[k].wait()
    for k in range(QUARTERS):
        at = pl.ds(k * quarter, quarter)
        g = gate_v[at, :].astype(f32)
        sig = jax.nn.sigmoid(g)
        h = hid_v[at, :].astype(f32) * tw[k * quarter : (k + 1) * quarter, :]
        raw = (h * up_v[at, :].astype(f32) * sig * (1.0 + g * (1.0 - sig))).astype(bf16)
        upo_ref[at, :] = h * g * sig
        go_ref[at, :] = raw
        g32[at, :] = raw.astype(f32)

    g_side = [
        push(g32.at[pl.ds(k * quarter, quarter), :], gr.at[1, pl.ds(k * quarter, quarter), :], (side, s))
        for k in range(QUARTERS)
    ]
    g_core = push(g32, gr.at[0], (core, s))

    local[6].wait()
    step = w_v.shape[0] // QUARTERS
    for k in range(QUARTERS):
        part[:, pl.ds(k * step, step)] = lax.dot_general(
            go_ref[pl.ds(0, rows), :], w_v[pl.ds(k * step, step), :],
            (((1,), (1,)), ((), ())), preferred_element_type=f32,
        )

    def block(index):
        return pl.ds(pl.multiple_of(index * tall, tall), tall)

    first = {}

    def send_first(delta, index):
        slot = len(first)
        first[delta] = (slot, push(part.at[block(index), :], rs1.at[slot], (r, near)))

    send_first(6, flip(flip(near, 2), 4))
    send_first(2, flip(near, 2))

    def absorb(delta, index):
        slot, copy = first[delta]
        copy.wait_recv()
        part[block(index), :] = part[block(index), :] + rs1[slot]

    def keep_x(group, slot, index):
        xo_ref[pl.ds(pl.multiple_of((group + 2) * rows + index * quarter, quarter), quarter), :] = (
            xq[group, slot].astype(bf16)
        )

    def keep_g(group, k):
        at = pl.ds(k * quarter, quarter)
        go_ref[pl.ds((group + 1) * rows + k * quarter, quarter), :] = gr[group, at, :].astype(bf16)

    def relay_g(k):
        at = pl.ds(k * quarter, quarter)
        g_side[k].wait_recv()
        copy = push(gr.at[1, at, :], gr.at[2, at, :], (core, s))
        keep_g(1, k)
        return copy

    x_near, x_mid = [], []
    for group, copy in enumerate((x_side, x_across)):
        copy.wait_recv()
        x_near.append(push(xq.at[group, 0], xq.at[group, 1], (r, near)))
        x_mid.append(push(xq.at[group, 0], xq.at[group, 2], (r, mid)))
    send_first(4, flip(near, 4))
    send_first(0, near)
    x_core.wait_recv()
    xo_ref[pl.ds(rows, rows), :] = xp[...].astype(bf16)
    g_core.wait_recv()
    for k in range(QUARTERS):
        keep_g(0, k)
    for group in range(2):
        keep_x(group, 0, q)
    for copy in counts:
        copy.wait_recv()
    total = (cnt[...] + cntr[0] + cntr[1] + cntr[2])[0:1, 0:1]
    scale = f32(rows * replicas) / total
    gs_ref[...] = jnp.broadcast_to(f32(rows) / total, gs_ref.shape)
    upo_ref[...] = upo_ref[...] * scale
    write(xo_ref.at[pl.ds(0, 2 * rows), :], xo_hbm.at[pl.ds(0, 2 * rows), :])
    write(go_ref.at[pl.ds(0, 2 * rows), :], go_hbm.at[pl.ds(0, 2 * rows), :])
    write(gs_ref, gs_hbm)
    write(upo_ref, upo_hbm)

    g_across = [relay_g(0)]
    absorb(6, flip(mid, 4))
    second_far = push(part.at[block(flip(mid, 4)), :], rs2.at[0], (r, mid))
    absorb(2, mid)
    second_own = push(part.at[block(mid), :], rs2.at[1], (r, mid))
    g_across.append(relay_g(1))
    g_across.append(relay_g(2))
    x_last = []
    for group in range(2):
        x_near[group].wait_recv()
        x_last.append(push(xq.at[group, 1], xq.at[group, 3], (r, mid)))
        keep_x(group, 1, lax.rem(near, QUARTERS))
    for group in range(2):
        x_mid[group].wait_recv()
        keep_x(group, 2, lax.rem(mid, QUARTERS))
    for k in range(2):
        g_across[k].wait_recv()
        keep_g(2, k)
    g_across.append(relay_g(3))
    write(go_ref.at[pl.ds(2 * rows, rows), :], go_hbm.at[pl.ds(2 * rows, rows), :])
    absorb(4, far)
    second_far.wait_recv()
    part[block(far), :] = part[block(far), :] + rs2[0]
    third = push(part.at[block(far), :], rs3, (r, far))
    for group in range(2):
        x_last[group].wait_recv()
        keep_x(group, 3, lax.rem(flip(near, 2), QUARTERS))
    write(xo_ref.at[pl.ds(2 * rows, 2 * rows), :], xo_hbm.at[pl.ds(2 * rows, 2 * rows), :])
    for k in range(2, QUARTERS):
        g_across[k].wait_recv()
        keep_g(2, k)
    write(go_ref.at[pl.ds(3 * rows, rows), :], go_hbm.at[pl.ds(3 * rows, rows), :])
    absorb(0, s)
    second_own.wait_recv()
    third.wait_recv()
    sum_ref[...] = (part[block(s), :] + rs2[1] + rs3[...]) * scale
    write(sum_ref, sum_hbm)
    for copy in started:
        copy.wait_send()
    for copy in written:
        copy.wait()


def exchange(inputs, gate_pre, up_pre, hidden_grad, segment_ids, doc_weight, w_gate):
    replicas, shards = lax.axis_size("replica"), lax.axis_size("shard")
    rows, features = inputs.shape
    hidden = gate_pre.shape[1]
    width, tall, quarter = features // replicas, rows // shards, rows // QUARTERS
    f32, bf16 = jnp.float32, jnp.bfloat16
    hbm = pl.BlockSpec(memory_space=pltpu.HBM)
    copies = 30
    return pl.pallas_call(
        exchange_kernel,
        out_shape=(
            jax.ShapeDtypeStruct((replicas * rows, width), bf16),
            jax.ShapeDtypeStruct((replicas * rows, hidden), bf16),
            jax.ShapeDtypeStruct((tall, features), f32),
            jax.ShapeDtypeStruct((rows, hidden), f32),
            jax.ShapeDtypeStruct((8, hidden), f32),
        ),
        in_specs=[hbm] * 7,
        out_specs=(hbm,) * 5,
        scratch_shapes=[
            pltpu.VMEM((replicas * rows, width), bf16),
            pltpu.VMEM((replicas * rows, hidden), bf16),
            pltpu.VMEM((tall, features), f32),
            pltpu.VMEM((rows, hidden), f32),
            pltpu.VMEM((8, hidden), f32),
            pltpu.VMEM((rows, features), bf16),
            pltpu.VMEM((rows, hidden), bf16),
            pltpu.VMEM((rows, hidden), bf16),
            pltpu.VMEM((rows, hidden), bf16),
            pltpu.VMEM(segment_ids.shape, jnp.int32),
            pltpu.VMEM(doc_weight.shape, jnp.int32),
            pltpu.VMEM((features, hidden), bf16),
            pltpu.VMEM((rows, features), f32),
            pltpu.VMEM((rows, hidden), f32),
            pltpu.VMEM((rows, features), f32),
            pltpu.VMEM((8, 128), f32),
            pltpu.VMEM((rows, width), f32),
            pltpu.VMEM((2, QUARTERS, quarter, width), f32),
            pltpu.VMEM((3, rows, hidden), f32),
            pltpu.VMEM((4, tall, features), f32),
            pltpu.VMEM((2, tall, features), f32),
            pltpu.VMEM((tall, features), f32),
            pltpu.VMEM((3, 8, 128), f32),
            pltpu.SemaphoreType.DMA((7,)),
            pltpu.SemaphoreType.DMA((8,)),
            pltpu.SemaphoreType.DMA((copies,)),
            pltpu.SemaphoreType.DMA((copies,)),
        ],
        compiler_params=pltpu.CompilerParams(
            collective_id=0, has_side_effects=True, vmem_limit_bytes=54 * 1024 * 1024
        ),
        cost_estimate=pl.CostEstimate(
            flops=2 * rows * hidden * features, bytes_accessed=40 * 1024 * 1024, transcendentals=0
        ),
        name="exchange",
    )(inputs, gate_pre, up_pre, hidden_grad, segment_ids, doc_weight, w_gate)


def step_kernel(
    x_hbm, g_hbm, sum_hbm, up_hbm, gs_hbm, ma_old, mo_old, se_old,
    ig_hbm, ug_hbm, ma_hbm, mo_hbm, se_hbm,
    x_ref, g_ref, sum_ref, up_ref, gs_ref, ma_ref, mo_ref, se_ref, ig_v, ug_v, ma_v, mo_v, se_v, isem, sems,
):
    band = ma_v.shape[1]
    written, loaded = [], []
    bands = [pl.ds(k * band, band) for k in range(ma_v.shape[0])]
    loads = [(g_hbm, g_ref), (x_hbm, x_ref), (gs_hbm, gs_ref)]
    for at in bands:
        loads += [
            (old.at[at, :], new.at[at, :])
            for old, new in ((mo_old, mo_ref), (se_old, se_ref), (ma_old, ma_ref))
        ]
    for k, (src, dst) in enumerate(loads + [(sum_hbm, sum_ref), (up_hbm, up_ref)]):
        copy = pltpu.make_async_copy(src, dst, isem.at[k])
        copy.start()
        loaded.append(copy)

    def write(src, dst):
        copy = pltpu.make_async_copy(src, dst, sems.at[len(written)])
        copy.start()
        written.append(copy)

    for copy in loaded[:3]:
        copy.wait()
    group_scale = gs_ref[0:1, :]
    for k, at in enumerate(bands):
        raw = lax.dot_general(
            x_ref[:, at], g_ref[...], (((0,), (0,)), ((), ())), preferred_element_type=jnp.float32
        )
        grad = raw * group_scale
        for copy in loaded[3 + 3 * k : 6 + 3 * k]:
            copy.wait()
        moment_new = 0.9 * mo_ref[at, :] + 0.1 * grad
        second_new = 0.95 * se_ref[at, :] + 0.05 * grad * grad
        mo_v[k] = moment_new
        se_v[k] = second_new
        master = ma_ref[at, :]
        first_fix = moment_new * (1.0 / (1.0 - 0.9**8))
        second_fix = second_new * (1.0 / (1.0 - 0.95**8))
        ma_v[k] = master - 0.003 * (first_fix / (jnp.sqrt(second_fix) + 1e-08) + 0.1 * master)
        write(mo_v.at[k], mo_hbm.at[at, :])
        write(se_v.at[k], se_hbm.at[at, :])
        write(ma_v.at[k], ma_hbm.at[at, :])
    for copy in loaded[3 + 3 * len(bands) :]:
        copy.wait()
    ig_v[...] = sum_ref[...].astype(ig_v.dtype)
    ug_v[...] = up_ref[...].astype(ug_v.dtype)
    write(ig_v, ig_hbm)
    write(ug_v, ug_hbm)
    for copy in written:
        copy.wait()


def step(x_all, gate_all, input_scaled, up_scaled, group_scale, master, moment, second):
    states = master.shape
    bands = 4
    f32, bf16 = jnp.float32, jnp.bfloat16
    hbm = pl.BlockSpec(memory_space=pltpu.HBM)
    banded = pltpu.VMEM((bands, states[0] // bands, states[1]), f32)
    return pl.pallas_call(
        step_kernel,
        out_shape=(
            jax.ShapeDtypeStruct(input_scaled.shape, bf16),
            jax.ShapeDtypeStruct(up_scaled.shape, bf16),
        )
        + (jax.ShapeDtypeStruct(states, f32),) * 3,
        in_specs=[hbm] * 8,
        out_specs=(hbm,) * 5,
        scratch_shapes=[
            pltpu.VMEM(x_all.shape, bf16),
            pltpu.VMEM(gate_all.shape, bf16),
            pltpu.VMEM(input_scaled.shape, f32),
            pltpu.VMEM(up_scaled.shape, f32),
            pltpu.VMEM(group_scale.shape, f32),
            pltpu.VMEM(states, f32),
            pltpu.VMEM(states, f32),
            pltpu.VMEM(states, f32),
            pltpu.VMEM(input_scaled.shape, bf16),
            pltpu.VMEM(up_scaled.shape, bf16),
            banded,
            banded,
            banded,
            pltpu.SemaphoreType.DMA((5 + 3 * bands,)),
            pltpu.SemaphoreType.DMA((2 + 3 * bands,)),
        ],
        compiler_params=pltpu.CompilerParams(vmem_limit_bytes=54 * 1024 * 1024),
        name="step",
    )(x_all, gate_all, input_scaled, up_scaled, group_scale, master, moment, second)


def gather_path(
    inputs, gate_pre, up_pre, hidden_grad, segment_ids, doc_weight, w_gate, master, moment, second
):
    factors = exchange(inputs, gate_pre, up_pre, hidden_grad, segment_ids, doc_weight, w_gate)
    return step(*factors, master, moment, second)


def on_device(*args):
    inputs, gate_pre = args[:2]
    replicas, shards = lax.axis_size("replica"), lax.axis_size("shard")
    rows, features = inputs.shape
    hidden = gate_pre.shape[1]
    gathered = replicas * rows * (features // replicas + hidden)
    fits = rows % (QUARTERS * 32) == 0 and features % (replicas * 128) == 0
    if (replicas, shards) == (4, 8) and fits and gathered <= features * hidden:
        return gather_path(*args)
    return reduce_path(*args)


def solution(mesh):
    in_specs = (
        P("replica", None),
        P("replica", "shard"),
        P("replica", "shard"),
        P("replica", "shard"),
        P("replica", None),
        P("replica", None),
        P(None, "shard"),
        P("replica", "shard"),
        P("replica", "shard"),
        P("replica", "shard"),
    )
    out_specs = (
        P(("replica", "shard"), None),
        P("replica", "shard"),
        P("replica", "shard"),
        P("replica", "shard"),
        P("replica", "shard"),
    )
    return jax.shard_map(
        on_device, mesh=mesh, in_specs=in_specs, out_specs=out_specs, check_vma=False
    )
```
